32 devices in a mesh: samp: 8 (over z, y), gene: 4 (over x, core).
Axes of the slice: x: 2, y: 2, z: 4, core: 2. Of those that a mesh axis runs over, the one named last changes fastest.
Arguments:
- genotypes: int32 [256, 4096], P('samp', 'gene'), may hold values from -2147483648 to 1789569706, as said below
- allele_freq: float32 [4096], P('gene'), may hold values from 0.035 to 0.56
- sample_weight: float32 [16, 256], P(None, 'samp'), may hold values from 0.2 to 2
- residual: float32 [16, 256], P(None, 'samp'), may hold values from -12 to 12
- variant_weight: float32 [4096], P('gene'), may hold values from 0.2 to 4
- block_gene: int32 [32], replicated, may hold values from 0 to 15, as said below
- gene_variants: int32 [16], replicated, may hold values from 1 to 384, as said below
Outputs:
- burden_z: float32 [16], replicated
- skat_z: float32 [16], replicated
The draws below stay inside these ranges and needn't reach their ends.
Inputs may be any that keep to these rules, and one draw needn't show every extreme that they name: Each word holds 16 dosages 0, 1 or 2: bits 2k and 2k+1 of genotypes[i, v] are the dosage of variant slot v in sample (k, i); a dosage 2 in the top field sets the sign bit. `block_gene`: never falling; the blocks come in aligned groups of four, each shared by two consecutive genes, so every gene has 1 to 3 blocks. `gene_variants`: A gene with m blocks has from (m - 1) * 128 + 1 to m * 128 live variants; the slots after them in its last block are padding.
All inputs are finite; a program needn't handle non-finite values.
Results may differ from the reference program's by a relative error of at most 0.0037.
Values sent between devices are 32-bit elements; how exact they have to be, the bound alone decides.
A program may use at most 64 MiB of HBM per device.

```python
import math
import jax
import jax.numpy as jnp
from jax import lax

FIELDS = 16
BLK = 128
ROWS = 256
SAMPLES = 4096
NBLK = 32
VARIANTS = 4096
NGENE = 16


def gene_layout(key):
    base = jax.random.fold_in(key, 11)
    groups = NBLK // 4
    split_at = jax.random.randint(jax.random.fold_in(base, 1), (groups,), 1, 4, dtype=jnp.int32)
    position = jnp.arange(4, dtype=jnp.int32)
    second = (position[None, :] >= split_at[:, None]).astype(jnp.int32)
    block_gene = (2 * jnp.arange(groups, dtype=jnp.int32)[:, None] + second).reshape(NBLK)
    gene_blocks = jnp.stack([split_at, 4 - split_at], axis=1).reshape(NGENE)
    tail_count = jax.random.randint(jax.random.fold_in(base, 2), (NGENE,), 1, BLK + 1, dtype=jnp.int32)
    return (block_gene, (gene_blocks - 1) * BLK + tail_count)


def draw_block_gene(key, part):
    return gene_layout(key)[0]


def draw_gene_variants(key, part):
    return gene_layout(key)[1]


def allele_levels(key):
    base = jax.random.fold_in(jax.random.fold_in(key, 21), 5)
    return jax.random.randint(base, (VARIANTS,), 40, 520, dtype=jnp.int32)


def draw_allele_freq(key, part):
    levels = allele_levels(key).astype(jnp.float32) / 1024.0
    return levels


def draw_genotypes(key, part):
    levels = allele_levels(key)
    base = jax.random.fold_in(key, 21)
    column = jnp.arange(VARIANTS, dtype=jnp.int32)

    def one_field(field_index, packed):
        field_key = jax.random.fold_in(base, field_index + 100)
        dosage = jnp.zeros((ROWS, VARIANTS), jnp.int32)
        for strand in range(2):
            strand_key = jax.random.fold_in(field_key, strand)
            fresh_bits = (jax.random.randint(jax.random.fold_in(strand_key, 1), (ROWS, VARIANTS), 0, 1024, dtype=jnp.int32) < levels[None, :]).astype(jnp.int32)
            restart = jax.random.randint(jax.random.fold_in(strand_key, 2), (ROWS, VARIANTS), 0, 5, dtype=jnp.int32) == 0
            restart = jnp.logical_or(restart, column[None, :] == 0)
            source = lax.cummax(jnp.where(restart, column[None, :], 0), axis=1)
            dosage = dosage + jnp.take_along_axis(fresh_bits, source, axis=1)
        return packed + jnp.left_shift(dosage, 2 * field_index)
    return lax.fori_loop(0, FIELDS, one_field, jnp.zeros((ROWS, VARIANTS), jnp.int32))


def draw_residual(key, part):
    row_index = jnp.arange(ROWS, dtype=jnp.float32)
    spread = 1.0 + row_index / ROWS
    values = jax.random.truncated_normal(key, -6.0, 6.0, (FIELDS, ROWS), jnp.float32)
    return values * spread[None, :]


def shard_levels(key, extent, shards, low, largest):
    gain, own = 1.0, jax.random.fold_in(key, 6)
    for dim, shards_of in shards:
        draws = jnp.exp(jax.random.uniform(jax.random.fold_in(own, dim), (shards_of,), jnp.float32, low / len(shards), largest / len(shards)))
        gain = gain * jnp.repeat(draws, extent[dim] // shards_of).reshape([-1 if axis == dim else 1 for axis in range(len(extent))])
    return gain


def setup_inputs(seed: int = 0) -> dict:
    streams_of = jax.random.split(jax.random.key(seed), 8)
    return {
        "genotypes": draw_genotypes(jax.random.fold_in(streams_of[7], 71), 0),
        "allele_freq": draw_allele_freq(jax.random.fold_in(streams_of[7], 71), 0),
        "sample_weight": jnp.clip(jnp.exp(math.log(2.0) - 2.3025851 * jax.random.uniform(streams_of[2], (FIELDS, ROWS), jnp.float32) ** shard_levels(streams_of[2], (FIELDS, ROWS), ((1, 8),), -0.2, 0.2)), 0.2, 2.0),
        "residual": draw_residual(jax.random.fold_in(streams_of[7], 71), 0),
        "variant_weight": jnp.clip(jnp.exp(math.log(4.0) - 2.9957323 * jax.random.uniform(streams_of[4], (VARIANTS,), jnp.float32) ** shard_levels(streams_of[4], (VARIANTS,), ((0, 4),), -0.2, 0.2)), 0.2, 4.0),
        "block_gene": draw_block_gene(jax.random.fold_in(streams_of[7], 71), 0),
        "gene_variants": draw_gene_variants(jax.random.fold_in(streams_of[7], 71), 0),
    }


def unpack(packed_words, allele_part, root_weight):
    offsets = 2 * jnp.arange(FIELDS, dtype=jnp.int32)
    dosage = jnp.bitwise_and(jnp.right_shift(packed_words[None, :, :], offsets[:, None, None]), 3)
    centered = dosage.astype(jnp.float32) - 2.0 * allele_part[None, None, :]
    return (root_weight[:, :, None] * centered).astype(jnp.bfloat16)

def block_stats(gram_part, scores, effective):
    weighted_score = effective * scores
    burden_sum = lax.optimization_barrier(jnp.sum(weighted_score, axis=1))
    skat_sum = lax.optimization_barrier(jnp.sum(weighted_score * weighted_score, axis=1))
    image = jnp.einsum('buv,bv->bu', gram_part, effective, precision=lax.Precision.HIGHEST)
    burden_var = lax.optimization_barrier(jnp.sum(effective * image, axis=1))
    diagonal = jnp.diagonal(gram_part, axis1=1, axis2=2)
    trace_one = lax.optimization_barrier(jnp.sum(effective * effective * diagonal, axis=1))
    scaled_gram = effective[:, :, None] * gram_part * effective[:, None, :]
    trace_two = lax.optimization_barrier(jnp.sum(scaled_gram * scaled_gram, axis=(1, 2)))
    return jnp.stack([burden_sum, burden_var, skat_sum, trace_one, trace_two])

def reference(genotypes, allele_freq, sample_weight, residual, variant_weight, block_gene, gene_variants):
    root_weight = jnp.sqrt(sample_weight)
    weighted_residual = (root_weight * residual).astype(jnp.bfloat16).reshape(1, FIELDS * ROWS)
    widened_residual = weighted_residual.astype(jnp.float32)
    variance = jnp.sum(sample_weight * residual * residual) / SAMPLES

    def block_terms(block_index):
        packed_words = lax.dynamic_slice_in_dim(genotypes, block_index * BLK, BLK, 1)
        allele_part = lax.dynamic_slice_in_dim(allele_freq, block_index * BLK, BLK, 0)
        scaled = unpack(packed_words, allele_part, root_weight).reshape(FIELDS * ROWS, BLK)
        widened = scaled.astype(jnp.float32)
        gram_part = jnp.dot(widened.T, widened, precision=lax.Precision.HIGHEST)
        score = jnp.dot(widened_residual, widened, precision=lax.Precision.HIGHEST)[0]
        return (gram_part, score)
    block_index = jnp.arange(NBLK, dtype=jnp.int32)
    gram_all, score_all = lax.map(block_terms, block_index)
    first_block = lax.optimization_barrier(jnp.sum((block_gene[None, :] < block_gene[:, None]).astype(jnp.int32), axis=1))
    counted = gene_variants[block_gene]
    column = jnp.arange(BLK, dtype=jnp.int32)
    is_live = (block_index - first_block)[:, None] * BLK + column[None, :] < counted[:, None]
    effective = variant_weight.reshape(NBLK, BLK) * is_live.astype(jnp.float32)
    stats = block_stats(gram_all, score_all, effective)
    member = (block_gene[:, None] == jnp.arange(NGENE, dtype=jnp.int32)[None, :]).astype(jnp.float32)
    totals = jnp.dot(stats, member, precision=lax.Precision.HIGHEST)
    burden_z = totals[0] / jnp.sqrt(variance * totals[1])
    skat_z = (totals[2] - variance * totals[3]) / (variance * jnp.sqrt(2.0 * totals[4]))
    return (burden_z, skat_z)
```

```python
import functools

import jax
import jax.numpy as jnp
from jax import lax
from jax.experimental import pallas as pl
from jax.experimental.pallas import tpu as pltpu
from jax.sharding import PartitionSpec as P

BLK = 128
MESH = pl.DeviceIdType.MESH
STATS = 5


def lane_sum(row):
    return jnp.sum(row, axis=1, keepdims=True)


def kernel(
    samp_size,
    gene_size,
    genotypes_hbm,
    freq_hbm,
    weight_hbm,
    residual_hbm,
    variant_hbm,
    block_gene_hbm,
    counts_hbm,
    burden_ref,
    skat_ref,
    words_in,
    freq_in,
    weight_in,
    residual_in,
    variant_in,
    block_gene_in,
    counts_in,
    tile_out,
    tiles,
    words,
    scaled,
    root_rows,
    residual_rows,
    pair_weight,
    row_out,
    rows,
    load_sem,
    send_sem,
    tile_sem,
    word_sem,
    row_send_sem,
    row_sem,
):
    devices = samp_size * gene_size
    samp = lax.axis_index("samp")
    gene = lax.axis_index("gene")
    me = samp * gene_size + gene
    fields, local_rows = weight_in.shape
    half = fields // 2
    group = BLK // local_rows
    chunks = samp_size // group
    owned = words.shape[1] // BLK
    local_blocks = freq_in.shape[0]
    genes = counts_in.shape[1]
    width = row_out.shape[1]

    def device_of(index):
        return {"samp": lax.div(index, gene_size), "gene": lax.rem(index, gene_size)}

    barrier = pltpu.get_barrier_semaphore()

    @pl.loop(1, devices)
    def _(step):
        pl.semaphore_signal(
            barrier,
            inc=1,
            device_id=device_of(lax.rem(me + step, devices)),
            device_id_type=MESH,
        )

    loads = [
        pltpu.make_async_copy(source, target, load_sem.at[place])
        for place, (source, target) in enumerate(
            (
                (weight_hbm, weight_in),
                (residual_hbm, residual_in),
                (genotypes_hbm, words_in),
                (freq_hbm, freq_in),
                (variant_hbm, variant_in),
                (block_gene_hbm, block_gene_in),
                (counts_hbm, counts_in),
            )
        )
    ]
    for load in loads:
        load.start()
    loads[0].wait()
    loads[1].wait()
    own_weight, own_residual = weight_in[...], residual_in[...]
    own_tile = jnp.concatenate(
        [own_weight[:half], own_weight[half:], own_residual[:half], own_residual[half:]], axis=1
    )
    tile_out[...] = own_tile
    tiles[samp] = own_tile
    for load in loads[2:]:
        load.wait()
    pl.semaphore_wait(barrier, devices - 1)

    def tile_copy(peer, slot):
        return pltpu.make_async_remote_copy(
            src_ref=tile_out,
            dst_ref=tiles.at[samp],
            send_sem=send_sem.at[0],
            recv_sem=tile_sem.at[slot],
            device_id={"samp": peer, "gene": gene},
            device_id_type=MESH,
        )

    def word_copy(peer, slot):
        start = pl.multiple_of(peer * (owned * BLK), BLK)
        return pltpu.make_async_remote_copy(
            src_ref=words_in.at[:, pl.ds(start, owned * BLK)],
            dst_ref=words.at[pl.ds(pl.multiple_of(samp * local_rows, local_rows), local_rows), :],
            send_sem=send_sem.at[1],
            recv_sem=word_sem.at[slot],
            device_id={"samp": peer, "gene": gene},
            device_id_type=MESH,
        )

    @pl.loop(1, samp_size)
    def _(step):
        tile_copy(lax.rem(samp + step, samp_size), samp).start()

    @pl.loop(1, samp_size)
    def _(step):
        word_copy(lax.rem(samp + step, samp_size), samp).start()

    own_start = pl.multiple_of(samp * (owned * BLK), BLK)
    own_place = pl.multiple_of(samp * local_rows, local_rows)
    words[pl.ds(own_place, local_rows), :] = words_in[:, pl.ds(own_start, owned * BLK)]

    block_gene = block_gene_in[...].astype(jnp.float32)
    counts = counts_in[...].astype(jnp.float32)
    block_lane = lax.broadcasted_iota(jnp.int32, block_gene.shape, 1)
    gene_lane = lax.broadcasted_iota(jnp.int32, counts.shape, 1).astype(jnp.float32)
    column = lax.broadcasted_iota(jnp.int32, (1, BLK), 1).astype(jnp.float32)
    stat_sub = lax.broadcasted_iota(jnp.int32, (8, width), 0)
    stat_lane = lax.broadcasted_iota(jnp.int32, (8, width), 1) - stat_sub * genes
    effective, places = [], []
    for block in range(owned):
        local_block = samp * owned + block
        block_id = gene * local_blocks + local_block
        gene_of = lane_sum(jnp.where(block_lane == block_id, block_gene, 0.0))
        first = lane_sum(jnp.where(block_gene < gene_of, 1.0, 0.0))
        counted = lane_sum(jnp.where(gene_lane == gene_of, counts, 0.0))
        block_float = jnp.zeros((1, 1), jnp.float32) + block_id.astype(jnp.float32)
        live = (block_float - first) * BLK + column < counted
        weights = jnp.where(live, variant_in[pl.ds(local_block, 1), :], 0.0)
        effective.append(weights)
        across = jnp.broadcast_to(weights, (BLK, BLK))
        pair_weight[block] = across * across.T
        member = stat_lane.astype(jnp.float32) == gene_of
        places.append(jnp.where(member & (stat_sub < STATS), 1.0, 0.0))

    def wait_tile(peer):
        pltpu.make_async_copy(tile_out, tiles.at[peer], tile_sem.at[peer]).wait()

    def wait_words(peer):
        place = words.at[pl.ds(pl.multiple_of(peer * local_rows, local_rows), local_rows), :]
        pltpu.make_async_copy(place, place, word_sem.at[peer]).wait()

    @pl.loop(1, samp_size)
    def _(step):
        wait_tile(lax.rem(samp + step, samp_size))

    power = jnp.zeros((half, BLK), jnp.float32)
    for chunk in range(chunks):
        parts = [tiles[chunk * group + peer] for peer in range(group)]
        kinds = [
            jnp.concatenate(
                [part[:, kind * local_rows : (kind + 1) * local_rows] for part in parts], axis=1
            )
            for kind in range(4)
        ]
        for upper in range(2):
            weight, resid = kinds[upper], kinds[2 + upper]
            root = jnp.sqrt(weight)
            power = power + weight * resid * resid
            root_rows[chunk, upper * half : (upper + 1) * half, :] = root
            residual_rows[chunk, upper * half : (upper + 1) * half, :] = root * resid
    variance = lane_sum(jnp.sum(power, axis=0, keepdims=True)) / (
        fields * local_rows * samp_size
    )

    @pl.loop(1, samp_size)
    def _(step):
        wait_words(lax.rem(samp + step, samp_size))

    message = jnp.zeros((8, width), jnp.float32)
    diagonal = lax.broadcasted_iota(jnp.int32, (BLK, BLK), 0) == lax.broadcasted_iota(
        jnp.int32, (BLK, BLK), 1
    )
    for block in range(owned):
        twice = 2.0 * jnp.broadcast_to(
            freq_in[pl.ds(samp * owned + block, 1), :], (BLK, BLK)
        ).T

        def chunk_gram(chunk, total, block=block, twice=twice):
            start = pl.multiple_of(chunk * BLK, BLK)
            turned = words[pl.ds(start, BLK), block * BLK : (block + 1) * BLK].T
            for field in range(fields):
                dosage = jnp.bitwise_and(jnp.right_shift(turned, 2 * field), 3)
                root = root_rows[chunk, field : field + 1, :]
                value = (root * (dosage.astype(jnp.float32) - twice)).astype(jnp.bfloat16)
                score = residual_rows[chunk, field : field + 1, :]
                lanes = slice(field * BLK, (field + 1) * BLK)
                scaled[:BLK, lanes] = value
                scaled[BLK:, lanes] = jnp.broadcast_to(score, (16, BLK)).astype(jnp.bfloat16)
            return total + lax.dot_general(
                scaled[...],
                scaled[:BLK, :],
                (((1,), (1,)), ((), ())),
                preferred_element_type=jnp.float32,
            )

        total = jnp.zeros((BLK + 16, BLK), jnp.float32)
        if chunks <= 2:
            for chunk in range(chunks):
                total = chunk_gram(chunk, total)
        else:
            total = lax.fori_loop(0, chunks, chunk_gram, total)
        weighted = total[:BLK] * pair_weight[block]
        score = effective[block] * total[BLK : BLK + 1]
        sums = [
            score,
            jnp.sum(weighted, axis=0, keepdims=True),
            score * score,
            jnp.sum(jnp.where(diagonal, weighted, 0.0), axis=0, keepdims=True),
            jnp.sum(weighted * weighted, axis=0, keepdims=True),
            jnp.zeros((8 - STATS, BLK), jnp.float32),
        ]
        message = message + lane_sum(jnp.concatenate(sums, axis=0)) * places[block]
    row = jnp.sum(message, axis=0, keepdims=True)
    row_out[...] = row
    rows[me] = row

    def row_copy(index):
        return pltpu.make_async_remote_copy(
            src_ref=row_out,
            dst_ref=rows.at[me],
            send_sem=row_send_sem,
            recv_sem=row_sem,
            device_id=device_of(index),
            device_id_type=MESH,
        )

    @pl.loop(1, devices)
    def _(step):
        row_copy(lax.rem(me + step, devices)).start()

    landed = rows.at[pl.ds(0, devices - 1)]
    pltpu.make_async_copy(landed, landed, row_sem).wait()
    totals = jnp.sum(rows[...], axis=0)
    parts = [totals[:, stat * genes : (stat + 1) * genes] for stat in range(STATS)]
    burden_ref[...] = parts[0] / jnp.sqrt(variance * parts[1])
    skat_ref[...] = (parts[2] - variance * parts[3]) / (
        variance * jnp.sqrt(2.0 * parts[4])
    )

    pltpu.make_async_copy(landed, landed, row_send_sem).wait()

    sent_tiles = tiles.at[pl.ds(0, samp_size - 1)]
    pltpu.make_async_copy(sent_tiles, sent_tiles, send_sem.at[0]).wait()
    sent_words = words.at[pl.ds(0, (samp_size - 1) * local_rows), :]
    pltpu.make_async_copy(sent_words, sent_words, send_sem.at[1]).wait()


def solution(mesh):
    samp_size, gene_size = mesh.shape["samp"], mesh.shape["gene"]
    devices = samp_size * gene_size

    def local(
        genotypes, allele_freq, sample_weight, residual, variant_weight, block_gene, gene_variants
    ):
        local_rows, columns = genotypes.shape
        local_blocks = columns // BLK
        owned = local_blocks // samp_size
        fields = sample_weight.shape[0]
        genes = gene_variants.shape[0]
        width = -(-STATS * genes // BLK) * BLK
        chunks = samp_size * local_rows // BLK
        burden, skat = pl.pallas_call(
            functools.partial(kernel, samp_size, gene_size),
            out_shape=[jax.ShapeDtypeStruct((1, genes), jnp.float32)] * 2,
            in_specs=[pl.BlockSpec(memory_space=pl.ANY)] * 7,
            out_specs=[pl.BlockSpec(memory_space=pltpu.VMEM)] * 2,
            scratch_shapes=[
                pltpu.VMEM((local_rows, columns), jnp.int32),
                pltpu.VMEM((local_blocks, BLK), jnp.float32),
                pltpu.VMEM((fields, local_rows), jnp.float32),
                pltpu.VMEM((fields, local_rows), jnp.float32),
                pltpu.VMEM((local_blocks, BLK), jnp.float32),
                pltpu.VMEM((1, block_gene.shape[0]), jnp.int32),
                pltpu.VMEM((1, genes), jnp.int32),
                pltpu.VMEM((fields // 2, 4 * local_rows), jnp.float32),
                pltpu.VMEM((samp_size, fields // 2, 4 * local_rows), jnp.float32),
                pltpu.VMEM((samp_size * local_rows, owned * BLK), jnp.int32),
                pltpu.VMEM((BLK + 16, fields * BLK), jnp.bfloat16),
                pltpu.VMEM((chunks, fields, BLK), jnp.float32),
                pltpu.VMEM((chunks, fields, BLK), jnp.float32),
                pltpu.VMEM((owned, BLK, BLK), jnp.float32),
                pltpu.VMEM((1, width), jnp.float32),
                pltpu.VMEM((devices, 1, width), jnp.float32),
                pltpu.SemaphoreType.DMA((7,)),
                pltpu.SemaphoreType.DMA((2,)),
                pltpu.SemaphoreType.DMA((samp_size,)),
                pltpu.SemaphoreType.DMA((samp_size,)),
                pltpu.SemaphoreType.DMA,
                pltpu.SemaphoreType.DMA,
            ],
            compiler_params=pltpu.CompilerParams(collective_id=0, has_side_effects=True),
        )(
            genotypes,
            allele_freq.reshape(local_blocks, BLK),
            sample_weight,
            residual,
            variant_weight.reshape(local_blocks, BLK),
            block_gene.reshape(1, -1),
            gene_variants.reshape(1, -1),
        )
        return burden.reshape(-1), skat.reshape(-1)

    placed = (P("samp", "gene"), P("gene"), P(None, "samp"), P(None, "samp"), P("gene"), P(), P())
    return jax.shard_map(local, mesh=mesh, in_specs=placed, out_specs=(P(), P()), check_vma=False)
```

```python
import functools

import jax
import jax.numpy as jnp
from jax import lax
from jax.experimental import pallas as pl
from jax.experimental.pallas import tpu as pltpu
from jax.sharding import PartitionSpec as P

BLK = 128
MESH = pl.DeviceIdType.MESH
STATS = 5


def lane_sum(row):
    return jnp.sum(row, axis=1, keepdims=True)


def kernel(
    samp_size,
    gene_size,
    genotypes_hbm,
    freq_hbm,
    weight_hbm,
    residual_hbm,
    variant_hbm,
    block_gene_hbm,
    counts_hbm,
    both_ref,
    words_in,
    freq_in,
    weight_in,
    residual_in,
    variant_in,
    block_gene_in,
    counts_in,
    tile_out,
    tiles,
    words,
    scaled,
    root_rows,
    residual_rows,
    power_rows,
    pair_weight,
    row_out,
    rows,
    load_sem,
    send_sem,
    tile_sem,
    word_sem,
    row_send_sem,
    row_sem,
    ready_sem,
    others_sem,
):
    devices = samp_size * gene_size
    samp = lax.axis_index("samp")
    gene = lax.axis_index("gene")
    me = samp * gene_size + gene
    fields, local_rows = weight_in.shape
    half = fields // 2
    group = BLK // local_rows
    chunks = samp_size // group
    owned = words.shape[1] // BLK
    local_blocks = freq_in.shape[0]
    genes = counts_in.shape[1]
    width = row_out.shape[1]

    loads = [
        pltpu.make_async_copy(source, target, load_sem.at[place])
        for place, (source, target) in enumerate(
            (
                (genotypes_hbm, words_in),
                (weight_hbm, weight_in),
                (residual_hbm, residual_in),
                (freq_hbm, freq_in),
                (variant_hbm, variant_in),
                (block_gene_hbm, block_gene_in),
                (counts_hbm, counts_in),
            )
        )
    ]
    for load in loads:
        load.start()

    def signal(semaphore, samp_to, gene_to):
        pl.semaphore_signal(
            semaphore,
            inc=1,
            device_id={"samp": samp_to, "gene": gene_to},
            device_id_type=MESH,
        )

    barrier = pltpu.get_barrier_semaphore()
    for gene_to in range(gene_size):

        @pl.when(gene_to > gene)
        def _(gene_to=gene_to):
            signal(barrier, samp, gene_to)

    @pl.loop(samp + 1, samp_size)
    def _(samp_to):
        for gene_to in range(gene_size):
            signal(barrier, samp_to, gene_to)

    loads[1].wait()
    loads[2].wait()
    own_weight, own_residual = weight_in[...], residual_in[...]
    own_tile = jnp.concatenate(
        [own_weight[:half], own_weight[half:], own_residual[:half], own_residual[half:]], axis=1
    )
    tile_out[...] = own_tile
    tiles[samp] = own_tile

    @pl.when(me > 0)
    def _():
        pl.semaphore_wait(barrier, me)

    @pl.loop(0, samp)
    def _(samp_to):
        signal(ready_sem.at[samp], samp_to, gene)

    loads[0].wait()

    def tile_copy(peer, slot):
        return pltpu.make_async_remote_copy(
            src_ref=tile_out,
            dst_ref=tiles.at[samp],
            send_sem=send_sem.at[0],
            recv_sem=tile_sem.at[slot],
            device_id={"samp": peer, "gene": gene},
            device_id_type=MESH,
        )

    def word_copy(peer, slot):
        start = pl.multiple_of(peer * (owned * BLK), BLK)
        return pltpu.make_async_remote_copy(
            src_ref=words_in.at[:, pl.ds(start, owned * BLK)],
            dst_ref=words.at[pl.ds(pl.multiple_of(samp * local_rows, local_rows), local_rows), :],
            send_sem=send_sem.at[1],
            recv_sem=word_sem.at[slot],
            device_id={"samp": peer, "gene": gene},
            device_id_type=MESH,
        )

    @pl.loop(0, samp)
    def _(peer):
        tile_copy(peer, samp).start()
        word_copy(peer, samp).start()

    for gene_to in range(gene_size):

        @pl.when(gene_to < gene)
        def _(gene_to=gene_to):
            signal(others_sem, samp, gene_to)

        @pl.when(gene_to != gene)
        def _(gene_to=gene_to):
            @pl.loop(0, samp)
            def _(samp_to):
                signal(others_sem, samp_to, gene_to)

    own_start = pl.multiple_of(samp * (owned * BLK), BLK)
    own_place = pl.multiple_of(samp * local_rows, local_rows)
    words[pl.ds(own_place, local_rows), :] = words_in[:, pl.ds(own_start, owned * BLK)]

    for load in loads[3:]:
        load.wait()
    block_gene = block_gene_in[...].astype(jnp.float32)
    counts = counts_in[...].astype(jnp.float32)
    block_lane = lax.broadcasted_iota(jnp.int32, block_gene.shape, 1)
    gene_lane = lax.broadcasted_iota(jnp.int32, counts.shape, 1).astype(jnp.float32)
    column = lax.broadcasted_iota(jnp.int32, (1, BLK), 1).astype(jnp.float32)
    stat_sub = lax.broadcasted_iota(jnp.int32, (8, width), 0)
    stat_lane = lax.broadcasted_iota(jnp.int32, (8, width), 1) - stat_sub * genes
    effective, places, twice = [], [], []
    for block in range(owned):
        local_block = samp * owned + block
        block_id = gene * local_blocks + local_block
        gene_of = lane_sum(jnp.where(block_lane == block_id, block_gene, 0.0))
        first = lane_sum(jnp.where(block_gene < gene_of, 1.0, 0.0))
        counted = lane_sum(jnp.where(gene_lane == gene_of, counts, 0.0))
        block_float = jnp.zeros((1, 1), jnp.float32) + block_id.astype(jnp.float32)
        live = (block_float - first) * BLK + column < counted
        weights = jnp.where(live, variant_in[pl.ds(local_block, 1), :], 0.0)
        effective.append(weights)
        across = jnp.broadcast_to(weights, (BLK, BLK))
        pair_weight[block] = across * across.T
        twice.append(2.0 * jnp.broadcast_to(freq_in[pl.ds(local_block, 1), :], (BLK, BLK)).T)
        member = stat_lane.astype(jnp.float32) == gene_of
        places.append(jnp.where(member & (stat_sub < STATS), 1.0, 0.0))

    def wait_tile(peer):
        pltpu.make_async_copy(tile_out, tiles.at[peer], tile_sem.at[peer]).wait()

    def wait_words(peer):
        place = words.at[pl.ds(pl.multiple_of(peer * local_rows, local_rows), local_rows), :]
        pltpu.make_async_copy(place, place, word_sem.at[peer]).wait()

    @pl.loop(samp + 1, samp_size)
    def _(peer):
        pl.semaphore_wait(ready_sem.at[peer], 1)
        tile_copy(peer, samp).start()
        word_copy(peer, samp).start()

    own_chunk = lax.div(samp, group)

    def add_chunk(step, totals):
        chunk = lax.rem(own_chunk + step, chunks)
        for place in range(group):

            @pl.when(chunk * group + place != samp)
            def _(peer=chunk * group + place):
                wait_tile(peer)

        parts = [tiles[chunk * group + place] for place in range(group)]
        kinds = [
            jnp.concatenate(
                [part[:, kind * local_rows : (kind + 1) * local_rows] for part in parts], axis=1
            )
            for kind in range(4)
        ]
        power = jnp.zeros((half, BLK), jnp.float32)
        for upper in range(2):
            weight, resid = kinds[upper], kinds[2 + upper]
            root = jnp.sqrt(weight)
            power = power + weight * resid * resid
            root_rows[upper * half : (upper + 1) * half, :] = root
            residual_rows[upper * half : (upper + 1) * half, :] = root * resid
        power_rows[chunk] = power
        for place in range(group):

            @pl.when(chunk * group + place != samp)
            def _(peer=chunk * group + place):
                wait_words(peer)

        start = pl.multiple_of(chunk * BLK, BLK)
        results = []
        for block in range(owned):
            turned = words[pl.ds(start, BLK), block * BLK : (block + 1) * BLK].T
            for field in range(fields):
                dosage = jnp.bitwise_and(jnp.right_shift(turned, 2 * field), 3)
                root = root_rows[field : field + 1, :]
                value = (root * (dosage.astype(jnp.float32) - twice[block])).astype(jnp.bfloat16)
                score = residual_rows[field : field + 1, :]
                lanes = slice(field * BLK, (field + 1) * BLK)
                scaled[:BLK, lanes] = value
                scaled[BLK:, lanes] = jnp.broadcast_to(score, (16, BLK)).astype(jnp.bfloat16)
            results.append(
                totals[block]
                + lax.dot_general(
                    scaled[...],
                    scaled[:BLK, :],
                    (((1,), (1,)), ((), ())),
                    preferred_element_type=jnp.float32,
                )
            )
        return tuple(results)

    totals = tuple(jnp.zeros((BLK + 16, BLK), jnp.float32) for _ in range(owned))
    if chunks <= 2:
        for step in range(chunks):
            totals = add_chunk(step, totals)
    else:
        totals = lax.fori_loop(0, chunks, add_chunk, totals)

    message = jnp.zeros((8, width), jnp.float32)
    diagonal = lax.broadcasted_iota(jnp.int32, (BLK, BLK), 0) == lax.broadcasted_iota(
        jnp.int32, (BLK, BLK), 1
    )
    for block in range(owned):
        total = totals[block]
        weighted = total[:BLK] * pair_weight[block]
        score = effective[block] * total[BLK : BLK + 1]
        sums = [
            score,
            jnp.sum(weighted, axis=0, keepdims=True),
            score * score,
            jnp.sum(jnp.where(diagonal, weighted, 0.0), axis=0, keepdims=True),
            jnp.sum(weighted * weighted, axis=0, keepdims=True),
            jnp.zeros((8 - STATS, BLK), jnp.float32),
        ]
        message = message + lane_sum(jnp.concatenate(sums, axis=0)) * places[block]
    row = jnp.sum(message, axis=0, keepdims=True)
    others = (samp_size - 1 - samp) * (gene_size - 1) + gene_size - 1 - gene

    @pl.when(others > 0)
    def _():
        pl.semaphore_wait(others_sem, others)

    row_out[...] = row
    rows[me] = row

    def row_copy(samp_to, gene_to):
        return pltpu.make_async_remote_copy(
            src_ref=row_out,
            dst_ref=rows.at[me],
            send_sem=row_send_sem,
            recv_sem=row_sem,
            device_id={"samp": samp_to, "gene": gene_to},
            device_id_type=MESH,
        )

    @pl.loop(1, samp_size)
    def _(step):
        samp_to = samp + step
        samp_to = jnp.where(samp_to >= samp_size, samp_to - samp_size, samp_to)
        for gene_to in range(gene_size):
            row_copy(samp_to, gene_to).start()

    for gene_to in range(gene_size):

        @pl.when(gene_to != gene)
        def _(gene_to=gene_to):
            row_copy(samp, gene_to).start()

    power = jnp.sum(power_rows[...], axis=0)
    variance = lane_sum(jnp.sum(power, axis=0, keepdims=True)) / (
        fields * local_rows * samp_size
    )
    landed = rows.at[pl.ds(0, devices - 1)]
    pltpu.make_async_copy(landed, landed, row_sem).wait()
    totals = jnp.sum(rows[...], axis=0)
    parts = [totals[:, stat * genes : (stat + 1) * genes] for stat in range(STATS)]
    both_ref[0:1] = parts[0] / jnp.sqrt(variance * parts[1])
    both_ref[1:2] = (parts[2] - variance * parts[3]) / (
        variance * jnp.sqrt(2.0 * parts[4])
    )

    pltpu.make_async_copy(landed, landed, row_send_sem).wait()

    sent_tiles = tiles.at[pl.ds(0, samp_size - 1)]
    pltpu.make_async_copy(sent_tiles, sent_tiles, send_sem.at[0]).wait()
    sent_words = words.at[pl.ds(0, (samp_size - 1) * local_rows), :]
    pltpu.make_async_copy(sent_words, sent_words, send_sem.at[1]).wait()


def solution(mesh):
    samp_size, gene_size = mesh.shape["samp"], mesh.shape["gene"]
    devices = samp_size * gene_size

    def local(
        genotypes, allele_freq, sample_weight, residual, variant_weight, block_gene, gene_variants
    ):
        local_rows, columns = genotypes.shape
        local_blocks = columns // BLK
        owned = local_blocks // samp_size
        fields = sample_weight.shape[0]
        genes = gene_variants.shape[0]
        width = -(-STATS * genes // BLK) * BLK
        chunks = samp_size * local_rows // BLK
        both = pl.pallas_call(
            functools.partial(kernel, samp_size, gene_size),
            out_shape=pltpu.VMEM((2, genes), jnp.float32),
            in_specs=[pl.BlockSpec(memory_space=pl.ANY)] * 7,
            out_specs=pl.BlockSpec(memory_space=pltpu.VMEM),
            scratch_shapes=[
                pltpu.VMEM((local_rows, columns), jnp.int32),
                pltpu.VMEM((local_blocks, BLK), jnp.float32),
                pltpu.VMEM((fields, local_rows), jnp.float32),
                pltpu.VMEM((fields, local_rows), jnp.float32),
                pltpu.VMEM((local_blocks, BLK), jnp.float32),
                pltpu.VMEM((1, block_gene.shape[0]), jnp.int32),
                pltpu.VMEM((1, genes), jnp.int32),
                pltpu.VMEM((fields // 2, 4 * local_rows), jnp.float32),
                pltpu.VMEM((samp_size, fields // 2, 4 * local_rows), jnp.float32),
                pltpu.VMEM((samp_size * local_rows, owned * BLK), jnp.int32),
                pltpu.VMEM((BLK + 16, fields * BLK), jnp.bfloat16),
                pltpu.VMEM((fields, BLK), jnp.float32),
                pltpu.VMEM((fields, BLK), jnp.float32),
                pltpu.VMEM((chunks, fields // 2, BLK), jnp.float32),
                pltpu.VMEM((owned, BLK, BLK), jnp.float32),
                pltpu.VMEM((1, width), jnp.float32),
                pltpu.VMEM((devices, 1, width), jnp.float32),
                pltpu.SemaphoreType.DMA((7,)),
                pltpu.SemaphoreType.DMA((2,)),
                pltpu.SemaphoreType.DMA((samp_size,)),
                pltpu.SemaphoreType.DMA((samp_size,)),
                pltpu.SemaphoreType.DMA,
                pltpu.SemaphoreType.DMA,
                pltpu.SemaphoreType.REGULAR((samp_size,)),
                pltpu.SemaphoreType.REGULAR,
            ],
            compiler_params=pltpu.CompilerParams(collective_id=0, has_side_effects=True),
        )(
            genotypes,
            allele_freq.reshape(local_blocks, BLK),
            sample_weight,
            residual,
            variant_weight.reshape(local_blocks, BLK),
            block_gene.reshape(1, -1),
            gene_variants.reshape(1, -1),
        )
        return both[0], both[1]

    placed = (P("samp", "gene"), P("gene"), P(None, "samp"), P(None, "samp"), P("gene"), P(), P())
    return jax.shard_map(local, mesh=mesh, in_specs=placed, out_specs=(P(), P()), check_vma=False)
```

```python
import functools

import jax
import jax.numpy as jnp
from jax import lax
from jax.experimental import pallas as pl
from jax.experimental.pallas import tpu as pltpu
from jax.sharding import PartitionSpec as P

BLK = 128
MESH = pl.DeviceIdType.MESH
STATS = 5


def lane_sum(row):
    return jnp.sum(row, axis=1, keepdims=True)


def kernel(
    samp_size,
    gene_size,
    genotypes_hbm,
    freq_hbm,
    weight_hbm,
    residual_hbm,
    variant_hbm,
    block_gene_hbm,
    counts_hbm,
    both_ref,
    words_in,
    freq_in,
    weight_in,
    residual_in,
    variant_in,
    block_gene_in,
    counts_in,
    tile_out,
    tiles,
    words,
    relay,
    scaled,
    root_rows,
    residual_rows,
    power_rows,
    pair_weight,
    row_out,
    rows,
    load_sem,
    tile_send_sem,
    word_send_sem,
    tile_sem,
    word_sem,
    relay_sem,
    row_send_sem,
    row_sem,
    ready_sem,
    others_sem,
):
    devices = samp_size * gene_size
    samp = lax.axis_index("samp")
    gene = lax.axis_index("gene")
    me = samp * gene_size + gene
    fields, local_rows = weight_in.shape
    half = fields // 2
    group = BLK // local_rows
    chunks = samp_size // group
    owned = words.shape[1] // BLK
    local_blocks = freq_in.shape[0]
    genes = counts_in.shape[1]
    width = row_out.shape[1]

    loads = [
        pltpu.make_async_copy(source, target, load_sem.at[place])
        for place, (source, target) in enumerate(
            (
                (genotypes_hbm, words_in),
                (weight_hbm, weight_in),
                (residual_hbm, residual_in),
                (freq_hbm, freq_in),
                (variant_hbm, variant_in),
                (block_gene_hbm, block_gene_in),
                (counts_hbm, counts_in),
            )
        )
    ]
    for load in loads:
        load.start()

    def signal(semaphore, samp_to, gene_to):
        pl.semaphore_signal(
            semaphore,
            inc=1,
            device_id={"samp": samp_to, "gene": gene_to},
            device_id_type=MESH,
        )

    barrier = pltpu.get_barrier_semaphore()
    for gene_to in range(gene_size):

        @pl.when(gene_to > gene)
        def _(gene_to=gene_to):
            signal(barrier, samp, gene_to)

    @pl.loop(samp + 1, samp_size)
    def _(samp_to):
        for gene_to in range(gene_size):
            signal(barrier, samp_to, gene_to)

    loads[1].wait()
    loads[2].wait()
    own_weight, own_residual = weight_in[...], residual_in[...]
    own_tile = jnp.concatenate(
        [own_weight[:half], own_weight[half:], own_residual[:half], own_residual[half:]], axis=1
    )
    tile_out[...] = own_tile
    tiles[samp] = own_tile

    @pl.when(me > 0)
    def _():
        pl.semaphore_wait(barrier, me)

    @pl.loop(0, samp)
    def _(samp_to):
        signal(ready_sem.at[samp], samp_to, gene)

    loads[0].wait()

    inner = 2 if samp_size % 2 == 0 else 1
    plane = lax.div(samp, inner)
    behind = samp - inner
    far_start = jnp.minimum((plane + 3) * inner, samp_size)
    forward_start = jnp.where(plane > 0, jnp.minimum((plane + 2) * inner, samp_size), samp_size)

    def place_of(peer):
        return words.at[pl.ds(pl.multiple_of(peer * local_rows, local_rows), local_rows), :]

    def columns_of(peer):
        return words_in.at[:, pl.ds(pl.multiple_of(peer * (owned * BLK), BLK), owned * BLK)]

    def remote(source, target, send, receive, peer):
        return pltpu.make_async_remote_copy(
            src_ref=source,
            dst_ref=target,
            send_sem=send,
            recv_sem=receive,
            device_id={"samp": peer, "gene": gene},
            device_id_type=MESH,
        )

    def tile_copy(peer):
        return remote(
            tile_out, tiles.at[samp], tile_send_sem.at[peer], tile_sem.at[samp], peer
        )

    def word_copy(peer):
        return remote(
            columns_of(peer), place_of(samp), word_send_sem.at[peer], word_sem.at[samp], peer
        )

    def relay_copy(peer):
        return remote(
            columns_of(peer),
            relay.at[peer],
            word_send_sem.at[peer],
            relay_sem.at[peer],
            samp + inner,
        )

    def forward_tile(peer):
        return remote(
            tiles.at[behind],
            tiles.at[behind],
            tile_send_sem.at[samp_size + peer],
            tile_sem.at[behind],
            peer,
        )

    def forward_words(peer):
        return remote(
            relay.at[peer],
            place_of(behind),
            word_send_sem.at[samp_size + peer],
            word_sem.at[behind],
            peer,
        )

    @pl.loop(0, samp)
    def _(peer):
        tile_copy(peer).start()
        word_copy(peer).start()

    for gene_to in range(gene_size):

        @pl.when(gene_to < gene)
        def _(gene_to=gene_to):
            signal(others_sem, samp, gene_to)

        @pl.when(gene_to != gene)
        def _(gene_to=gene_to):
            @pl.loop(0, samp)
            def _(samp_to):
                signal(others_sem, samp_to, gene_to)

    own_start = pl.multiple_of(samp * (owned * BLK), BLK)
    own_place = pl.multiple_of(samp * local_rows, local_rows)
    words[pl.ds(own_place, local_rows), :] = words_in[:, pl.ds(own_start, owned * BLK)]

    for load in loads[3:]:
        load.wait()
    block_gene = block_gene_in[...].astype(jnp.float32)
    counts = counts_in[...].astype(jnp.float32)
    block_lane = lax.broadcasted_iota(jnp.int32, block_gene.shape, 1)
    gene_lane = lax.broadcasted_iota(jnp.int32, counts.shape, 1).astype(jnp.float32)
    column = lax.broadcasted_iota(jnp.int32, (1, BLK), 1).astype(jnp.float32)
    stat_sub = lax.broadcasted_iota(jnp.int32, (8, width), 0)
    stat_lane = lax.broadcasted_iota(jnp.int32, (8, width), 1) - stat_sub * genes
    effective, places, twice = [], [], []
    for block in range(owned):
        local_block = samp * owned + block
        block_id = gene * local_blocks + local_block
        gene_of = lane_sum(jnp.where(block_lane == block_id, block_gene, 0.0))
        first = lane_sum(jnp.where(block_gene < gene_of, 1.0, 0.0))
        counted = lane_sum(jnp.where(gene_lane == gene_of, counts, 0.0))
        block_float = jnp.zeros((1, 1), jnp.float32) + block_id.astype(jnp.float32)
        live = (block_float - first) * BLK + column < counted
        weights = jnp.where(live, variant_in[pl.ds(local_block, 1), :], 0.0)
        effective.append(weights)
        across = jnp.broadcast_to(weights, (BLK, BLK))
        pair_weight[block] = across * across.T
        twice.append(2.0 * jnp.broadcast_to(freq_in[pl.ds(local_block, 1), :], (BLK, BLK)).T)
        member = stat_lane.astype(jnp.float32) == gene_of
        places.append(jnp.where(member & (stat_sub < STATS), 1.0, 0.0))

    def wait_tile(peer):
        pltpu.make_async_copy(tile_out, tiles.at[peer], tile_sem.at[peer]).wait()

    def wait_words(peer):
        place = place_of(peer)
        pltpu.make_async_copy(place, place, word_sem.at[peer]).wait()

    @pl.when(plane > 0)
    def _():
        wait_tile(behind)

    @pl.loop(samp + 1, far_start)
    def _(peer):
        pl.semaphore_wait(ready_sem.at[peer], 1)

        @pl.when(peer >= forward_start)
        def _():
            forward_tile(peer).start()
            pltpu.make_async_copy(relay.at[peer], relay.at[peer], relay_sem.at[peer]).wait()
            forward_words(peer).start()

        tile_copy(peer).start()
        word_copy(peer).start()

        @pl.when(peer == samp + inner)
        def _():
            @pl.loop(far_start, samp_size)
            def _(far):
                relay_copy(far).start()

    @pl.loop(far_start, samp_size)
    def _(peer):
        @pl.when(peer >= forward_start)
        def _():
            pl.semaphore_wait(ready_sem.at[peer], 1)
            forward_tile(peer).start()
            pltpu.make_async_copy(relay.at[peer], relay.at[peer], relay_sem.at[peer]).wait()
            forward_words(peer).start()

    own_chunk = lax.div(samp, group)

    def add_chunk(step, totals):
        chunk = lax.rem(own_chunk + step, chunks)
        for place in range(group):

            @pl.when((chunk * group + place != samp) & (chunk * group + place != behind))
            def _(peer=chunk * group + place):
                wait_tile(peer)

        parts = [tiles[chunk * group + place] for place in range(group)]
        kinds = [
            jnp.concatenate(
                [part[:, kind * local_rows : (kind + 1) * local_rows] for part in parts], axis=1
            )
            for kind in range(4)
        ]
        power = jnp.zeros((half, BLK), jnp.float32)
        for upper in range(2):
            weight, resid = kinds[upper], kinds[2 + upper]
            root = jnp.sqrt(weight)
            power = power + weight * resid * resid
            root_rows[upper * half : (upper + 1) * half, :] = root
            residual_rows[upper * half : (upper + 1) * half, :] = root * resid
        power_rows[chunk] = power
        for place in range(group):

            @pl.when(chunk * group + place != samp)
            def _(peer=chunk * group + place):
                wait_words(peer)

        start = pl.multiple_of(chunk * BLK, BLK)
        results = []
        for block in range(owned):
            turned = words[pl.ds(start, BLK), block * BLK : (block + 1) * BLK].T
            for field in range(fields):
                dosage = jnp.bitwise_and(jnp.right_shift(turned, 2 * field), 3)
                root = root_rows[field : field + 1, :]
                value = (root * (dosage.astype(jnp.float32) - twice[block])).astype(jnp.bfloat16)
                score = residual_rows[field : field + 1, :]
                lanes = slice(field * BLK, (field + 1) * BLK)
                scaled[:BLK, lanes] = value
                scaled[BLK:, lanes] = jnp.broadcast_to(score, (16, BLK)).astype(jnp.bfloat16)
            results.append(
                totals[block]
                + lax.dot_general(
                    scaled[...],
                    scaled[:BLK, :],
                    (((1,), (1,)), ((), ())),
                    preferred_element_type=jnp.float32,
                )
            )
        return tuple(results)

    totals = tuple(jnp.zeros((BLK + 16, BLK), jnp.float32) for _ in range(owned))
    if chunks <= 2:
        for step in range(chunks):
            totals = add_chunk(step, totals)
    else:
        totals = lax.fori_loop(0, chunks, add_chunk, totals)

    message = jnp.zeros((8, width), jnp.float32)
    diagonal = lax.broadcasted_iota(jnp.int32, (BLK, BLK), 0) == lax.broadcasted_iota(
        jnp.int32, (BLK, BLK), 1
    )
    for block in range(owned):
        total = totals[block]
        weighted = total[:BLK] * pair_weight[block]
        score = effective[block] * total[BLK : BLK + 1]
        sums = [
            score,
            jnp.sum(weighted, axis=0, keepdims=True),
            score * score,
            jnp.sum(jnp.where(diagonal, weighted, 0.0), axis=0, keepdims=True),
            jnp.sum(weighted * weighted, axis=0, keepdims=True),
            jnp.zeros((8 - STATS, BLK), jnp.float32),
        ]
        message = message + lane_sum(jnp.concatenate(sums, axis=0)) * places[block]
    row = jnp.sum(message, axis=0, keepdims=True)
    @pl.loop(far_start, samp_size)
    def _(peer):
        @pl.when(plane == 0)
        def _():
            pl.semaphore_wait(ready_sem.at[peer], 1)

    others = (samp_size - 1 - samp) * (gene_size - 1) + gene_size - 1 - gene

    @pl.when(others > 0)
    def _():
        pl.semaphore_wait(others_sem, others)

    row_out[...] = row
    rows[me] = row

    def row_copy(samp_to, gene_to):
        return pltpu.make_async_remote_copy(
            src_ref=row_out,
            dst_ref=rows.at[me],
            send_sem=row_send_sem,
            recv_sem=row_sem,
            device_id={"samp": samp_to, "gene": gene_to},
            device_id_type=MESH,
        )

    @pl.loop(1, samp_size)
    def _(step):
        gap = samp_size - step

        @pl.when(samp + gap < samp_size)
        def _():
            for gene_to in range(gene_size):
                row_copy(samp + gap, gene_to).start()

        @pl.when(samp - gap >= 0)
        def _():
            for gene_to in range(gene_size):
                row_copy(samp - gap, gene_to).start()

    for gene_to in range(gene_size):

        @pl.when(gene_to != gene)
        def _(gene_to=gene_to):
            row_copy(samp, gene_to).start()

    power = jnp.sum(power_rows[...], axis=0)
    variance = lane_sum(jnp.sum(power, axis=0, keepdims=True)) / (
        fields * local_rows * samp_size
    )
    landed = rows.at[pl.ds(0, devices - 1)]
    pltpu.make_async_copy(landed, landed, row_sem).wait()
    totals = jnp.sum(rows[...], axis=0)
    parts = [totals[:, stat * genes : (stat + 1) * genes] for stat in range(STATS)]
    both_ref[0:1] = parts[0] / jnp.sqrt(variance * parts[1])
    both_ref[1:2] = (parts[2] - variance * parts[3]) / (
        variance * jnp.sqrt(2.0 * parts[4])
    )

    pltpu.make_async_copy(landed, landed, row_send_sem).wait()

    @pl.loop(0, samp_size)
    def _(peer):
        @pl.when((peer != samp) & (peer < far_start))
        def _():
            tile_copy(peer).wait_send()

        @pl.when(peer != samp)
        def _():
            word_copy(peer).wait_send()

        @pl.when(peer >= forward_start)
        def _():
            forward_tile(peer).wait_send()
            forward_words(peer).wait_send()


def solution(mesh):
    samp_size, gene_size = mesh.shape["samp"], mesh.shape["gene"]
    devices = samp_size * gene_size

    def local(
        genotypes, allele_freq, sample_weight, residual, variant_weight, block_gene, gene_variants
    ):
        local_rows, columns = genotypes.shape
        local_blocks = columns // BLK
        owned = local_blocks // samp_size
        fields = sample_weight.shape[0]
        genes = gene_variants.shape[0]
        width = -(-STATS * genes // BLK) * BLK
        chunks = samp_size * local_rows // BLK
        both = pl.pallas_call(
            functools.partial(kernel, samp_size, gene_size),
            out_shape=pltpu.VMEM((2, genes), jnp.float32),
            in_specs=[pl.BlockSpec(memory_space=pl.ANY)] * 7,
            out_specs=pl.BlockSpec(memory_space=pltpu.VMEM),
            scratch_shapes=[
                pltpu.VMEM((local_rows, columns), jnp.int32),
                pltpu.VMEM((local_blocks, BLK), jnp.float32),
                pltpu.VMEM((fields, local_rows), jnp.float32),
                pltpu.VMEM((fields, local_rows), jnp.float32),
                pltpu.VMEM((local_blocks, BLK), jnp.float32),
                pltpu.VMEM((1, block_gene.shape[0]), jnp.int32),
                pltpu.VMEM((1, genes), jnp.int32),
                pltpu.VMEM((fields // 2, 4 * local_rows), jnp.float32),
                pltpu.VMEM((samp_size, fields // 2, 4 * local_rows), jnp.float32),
                pltpu.VMEM((samp_size * local_rows, owned * BLK), jnp.int32),
                pltpu.VMEM((samp_size, local_rows, owned * BLK), jnp.int32),
                pltpu.VMEM((BLK + 16, fields * BLK), jnp.bfloat16),
                pltpu.VMEM((fields, BLK), jnp.float32),
                pltpu.VMEM((fields, BLK), jnp.float32),
                pltpu.VMEM((chunks, fields // 2, BLK), jnp.float32),
                pltpu.VMEM((owned, BLK, BLK), jnp.float32),
                pltpu.VMEM((1, width), jnp.float32),
                pltpu.VMEM((devices, 1, width), jnp.float32),
                pltpu.SemaphoreType.DMA((7,)),
                pltpu.SemaphoreType.DMA((2 * samp_size,)),
                pltpu.SemaphoreType.DMA((2 * samp_size,)),
                pltpu.SemaphoreType.DMA((samp_size,)),
                pltpu.SemaphoreType.DMA((samp_size,)),
                pltpu.SemaphoreType.DMA((samp_size,)),
                pltpu.SemaphoreType.DMA,
                pltpu.SemaphoreType.DMA,
                pltpu.SemaphoreType.REGULAR((samp_size,)),
                pltpu.SemaphoreType.REGULAR,
            ],
            compiler_params=pltpu.CompilerParams(collective_id=0, has_side_effects=True),
        )(
            genotypes,
            allele_freq.reshape(local_blocks, BLK),
            sample_weight,
            residual,
            variant_weight.reshape(local_blocks, BLK),
            block_gene.reshape(1, -1),
            gene_variants.reshape(1, -1),
        )
        return both[0], both[1]

    placed = (P("samp", "gene"), P("gene"), P(None, "samp"), P(None, "samp"), P("gene"), P(), P())
    return jax.shard_map(local, mesh=mesh, in_specs=placed, out_specs=(P(), P()), check_vma=False)
```

```python
import functools

import jax
import jax.numpy as jnp
from jax import lax
from jax.experimental import pallas as pl
from jax.experimental.pallas import tpu as pltpu
from jax.sharding import PartitionSpec as P

BLK = 128
MESH = pl.DeviceIdType.MESH
STATS = 5


def lane_sum(row):
    return jnp.sum(row, axis=1, keepdims=True)


def kernel(
    samp_size,
    gene_size,
    genotypes_hbm,
    freq_hbm,
    weight_hbm,
    residual_hbm,
    variant_hbm,
    block_gene_hbm,
    counts_hbm,
    both_ref,
    words_in,
    freq_in,
    weight_in,
    residual_in,
    variant_in,
    block_gene_in,
    counts_in,
    tile_out,
    tiles,
    words,
    scaled,
    root_rows,
    residual_rows,
    power_rows,
    pair_weight,
    row_out,
    rows,
    load_sem,
    send_sem,
    tile_sem,
    word_sem,
    row_send_sem,
    row_sem,
    ready_sem,
    others_sem,
):
    devices = samp_size * gene_size
    samp = lax.axis_index("samp")
    gene = lax.axis_index("gene")
    me = samp * gene_size + gene
    fields, local_rows = weight_in.shape
    half = fields // 2
    group = BLK // local_rows
    chunks = samp_size // group
    owned = words.shape[1] // BLK
    local_blocks = freq_in.shape[0]
    genes = counts_in.shape[1]
    width = row_out.shape[1]

    loads = [
        pltpu.make_async_copy(source, target, load_sem.at[place])
        for place, (source, target) in enumerate(
            (
                (genotypes_hbm, words_in),
                (weight_hbm, weight_in),
                (residual_hbm, residual_in),
                (freq_hbm, freq_in),
                (variant_hbm, variant_in),
                (block_gene_hbm, block_gene_in),
                (counts_hbm, counts_in),
            )
        )
    ]
    for load in loads:
        load.start()

    def signal(semaphore, samp_to, gene_to):
        pl.semaphore_signal(
            semaphore,
            inc=1,
            device_id={"samp": samp_to, "gene": gene_to},
            device_id_type=MESH,
        )

    barrier = pltpu.get_barrier_semaphore()
    for gene_to in range(gene_size):

        @pl.when(gene_to > gene)
        def _(gene_to=gene_to):
            signal(barrier, samp, gene_to)

    @pl.loop(samp + 1, samp_size)
    def _(samp_to):
        for gene_to in range(gene_size):
            signal(barrier, samp_to, gene_to)

    loads[1].wait()
    loads[2].wait()
    own_weight, own_residual = weight_in[...], residual_in[...]
    own_tile = jnp.concatenate(
        [own_weight[:half], own_weight[half:], own_residual[:half], own_residual[half:]], axis=1
    )
    tile_out[...] = own_tile
    tiles[samp] = own_tile

    @pl.when(me > 0)
    def _():
        pl.semaphore_wait(barrier, me)

    @pl.loop(0, samp)
    def _(samp_to):
        signal(ready_sem.at[samp], samp_to, gene)

    def tile_copy(peer, slot):
        return pltpu.make_async_remote_copy(
            src_ref=tile_out,
            dst_ref=tiles.at[samp],
            send_sem=send_sem.at[0],
            recv_sem=tile_sem.at[slot],
            device_id={"samp": peer, "gene": gene},
            device_id_type=MESH,
        )

    def word_copy(peer, slot):
        start = pl.multiple_of(peer * (owned * BLK), BLK)
        return pltpu.make_async_remote_copy(
            src_ref=words_in.at[:, pl.ds(start, owned * BLK)],
            dst_ref=words.at[pl.ds(pl.multiple_of(samp * local_rows, local_rows), local_rows), :],
            send_sem=send_sem.at[1],
            recv_sem=word_sem.at[slot],
            device_id={"samp": peer, "gene": gene},
            device_id_type=MESH,
        )

    @pl.loop(0, samp)
    def _(peer):
        tile_copy(peer, samp).start()

    loads[0].wait()

    @pl.loop(0, samp)
    def _(peer):
        word_copy(peer, samp).start()

    for gene_to in range(gene_size):

        @pl.when(gene_to < gene)
        def _(gene_to=gene_to):
            signal(others_sem, samp, gene_to)

        @pl.when(gene_to != gene)
        def _(gene_to=gene_to):
            @pl.loop(0, samp)
            def _(samp_to):
                signal(others_sem, samp_to, gene_to)

    own_start = pl.multiple_of(samp * (owned * BLK), BLK)
    own_place = pl.multiple_of(samp * local_rows, local_rows)
    words[pl.ds(own_place, local_rows), :] = words_in[:, pl.ds(own_start, owned * BLK)]

    for load in loads[3:]:
        load.wait()
    block_gene = block_gene_in[...].astype(jnp.float32)
    counts = counts_in[...].astype(jnp.float32)
    block_lane = lax.broadcasted_iota(jnp.int32, block_gene.shape, 1)
    gene_lane = lax.broadcasted_iota(jnp.int32, counts.shape, 1).astype(jnp.float32)
    column = lax.broadcasted_iota(jnp.int32, (1, BLK), 1).astype(jnp.float32)
    stat_sub = lax.broadcasted_iota(jnp.int32, (8, width), 0)
    stat_lane = lax.broadcasted_iota(jnp.int32, (8, width), 1) - stat_sub * genes
    effective, places, twice = [], [], []
    for block in range(owned):
        local_block = samp * owned + block
        block_id = gene * local_blocks + local_block
        gene_of = lane_sum(jnp.where(block_lane == block_id, block_gene, 0.0))
        first = lane_sum(jnp.where(block_gene < gene_of, 1.0, 0.0))
        counted = lane_sum(jnp.where(gene_lane == gene_of, counts, 0.0))
        block_float = jnp.zeros((1, 1), jnp.float32) + block_id.astype(jnp.float32)
        live = (block_float - first) * BLK + column < counted
        weights = jnp.where(live, variant_in[pl.ds(local_block, 1), :], 0.0)
        effective.append(weights)
        across = jnp.broadcast_to(weights, (BLK, BLK))
        pair_weight[block] = across * across.T
        twice.append(2.0 * jnp.broadcast_to(freq_in[pl.ds(local_block, 1), :], (BLK, BLK)).T)
        member = stat_lane.astype(jnp.float32) == gene_of
        places.append(jnp.where(member & (stat_sub < STATS), 1.0, 0.0))

    def wait_tile(peer):
        pltpu.make_async_copy(tile_out, tiles.at[peer], tile_sem.at[peer]).wait()

    def wait_words(peer):
        place = words.at[pl.ds(pl.multiple_of(peer * local_rows, local_rows), local_rows), :]
        pltpu.make_async_copy(place, place, word_sem.at[peer]).wait()

    @pl.loop(samp + 1, samp_size)
    def _(peer):
        pl.semaphore_wait(ready_sem.at[peer], 1)
        tile_copy(peer, samp).start()
        word_copy(peer, samp).start()

    own_chunk = lax.div(samp, group)

    def add_chunk(step, totals):
        chunk = lax.rem(own_chunk + step, chunks)
        for place in range(group):

            @pl.when(chunk * group + place != samp)
            def _(peer=chunk * group + place):
                wait_tile(peer)

        parts = [tiles[chunk * group + place] for place in range(group)]
        kinds = [
            jnp.concatenate(
                [part[:, kind * local_rows : (kind + 1) * local_rows] for part in parts], axis=1
            )
            for kind in range(4)
        ]
        power = jnp.zeros((half, BLK), jnp.float32)
        for upper in range(2):
            weight, resid = kinds[upper], kinds[2 + upper]
            root = jnp.sqrt(weight)
            power = power + weight * resid * resid
            root_rows[upper * half : (upper + 1) * half, :] = root
            residual_rows[upper * half : (upper + 1) * half, :] = root * resid
        power_rows[chunk] = power
        for place in range(group):

            @pl.when(chunk * group + place != samp)
            def _(peer=chunk * group + place):
                wait_words(peer)

        start = pl.multiple_of(chunk * BLK, BLK)
        results = []
        for block in range(owned):
            turned = words[pl.ds(start, BLK), block * BLK : (block + 1) * BLK].T
            for field in range(fields):
                dosage = jnp.bitwise_and(jnp.right_shift(turned, 2 * field), 3)
                root = root_rows[field : field + 1, :]
                value = (root * (dosage.astype(jnp.float32) - twice[block])).astype(jnp.bfloat16)
                score = residual_rows[field : field + 1, :]
                lanes = slice(field * BLK, (field + 1) * BLK)
                scaled[:BLK, lanes] = value
                scaled[BLK:, lanes] = jnp.broadcast_to(score, (16, BLK)).astype(jnp.bfloat16)
            results.append(
                totals[block]
                + lax.dot_general(
                    scaled[...],
                    scaled[:BLK, :],
                    (((1,), (1,)), ((), ())),
                    preferred_element_type=jnp.float32,
                )
            )
        return tuple(results)

    totals = tuple(jnp.zeros((BLK + 16, BLK), jnp.float32) for _ in range(owned))
    if chunks <= 2:
        for step in range(chunks):
            totals = add_chunk(step, totals)
    else:
        totals = lax.fori_loop(0, chunks, add_chunk, totals)

    message = jnp.zeros((8, width), jnp.float32)
    diagonal = lax.broadcasted_iota(jnp.int32, (BLK, BLK), 0) == lax.broadcasted_iota(
        jnp.int32, (BLK, BLK), 1
    )
    for block in range(owned):
        total = totals[block]
        weighted = total[:BLK] * pair_weight[block]
        score = effective[block] * total[BLK : BLK + 1]
        sums = [
            score,
            jnp.sum(weighted, axis=0, keepdims=True),
            score * score,
            jnp.sum(jnp.where(diagonal, weighted, 0.0), axis=0, keepdims=True),
            jnp.sum(weighted * weighted, axis=0, keepdims=True),
            jnp.zeros((8 - STATS, BLK), jnp.float32),
        ]
        message = message + lane_sum(jnp.concatenate(sums, axis=0)) * places[block]
    row = jnp.sum(message, axis=0, keepdims=True)
    others = (samp_size - 1 - samp) * (gene_size - 1) + gene_size - 1 - gene

    @pl.when(others > 0)
    def _():
        pl.semaphore_wait(others_sem, others)

    row_out[...] = row
    rows[me] = row

    def row_copy(samp_to, gene_to):
        return pltpu.make_async_remote_copy(
            src_ref=row_out,
            dst_ref=rows.at[me],
            send_sem=row_send_sem,
            recv_sem=row_sem,
            device_id={"samp": samp_to, "gene": gene_to},
            device_id_type=MESH,
        )

    @pl.loop(1, samp_size)
    def _(step):
        gap = samp_size - step

        @pl.when(samp + gap < samp_size)
        def _():
            for gene_to in range(gene_size):
                row_copy(samp + gap, gene_to).start()

        @pl.when(samp - gap >= 0)
        def _():
            for gene_to in range(gene_size):
                row_copy(samp - gap, gene_to).start()

    for gene_to in range(gene_size):

        @pl.when(gene_to != gene)
        def _(gene_to=gene_to):
            row_copy(samp, gene_to).start()

    power = jnp.sum(power_rows[...], axis=0)
    variance = lane_sum(jnp.sum(power, axis=0, keepdims=True)) / (
        fields * local_rows * samp_size
    )
    landed = rows.at[pl.ds(0, devices - 1)]
    pltpu.make_async_copy(landed, landed, row_sem).wait()
    totals = jnp.sum(rows[...], axis=0)
    parts = [totals[:, stat * genes : (stat + 1) * genes] for stat in range(STATS)]
    both_ref[0:1] = parts[0] / jnp.sqrt(variance * parts[1])
    both_ref[1:2] = (parts[2] - variance * parts[3]) / (
        variance * jnp.sqrt(2.0 * parts[4])
    )

    pltpu.make_async_copy(landed, landed, row_send_sem).wait()

    sent_tiles = tiles.at[pl.ds(0, samp_size - 1)]
    pltpu.make_async_copy(sent_tiles, sent_tiles, send_sem.at[0]).wait()
    sent_words = words.at[pl.ds(0, (samp_size - 1) * local_rows), :]
    pltpu.make_async_copy(sent_words, sent_words, send_sem.at[1]).wait()


def solution(mesh):
    samp_size, gene_size = mesh.shape["samp"], mesh.shape["gene"]
    devices = samp_size * gene_size

    def local(
        genotypes, allele_freq, sample_weight, residual, variant_weight, block_gene, gene_variants
    ):
        local_rows, columns = genotypes.shape
        local_blocks = columns // BLK
        owned = local_blocks // samp_size
        fields = sample_weight.shape[0]
        genes = gene_variants.shape[0]
        width = -(-STATS * genes // BLK) * BLK
        chunks = samp_size * local_rows // BLK
        both = pl.pallas_call(
            functools.partial(kernel, samp_size, gene_size),
            out_shape=pltpu.VMEM((2, genes), jnp.float32),
            in_specs=[pl.BlockSpec(memory_space=pl.ANY)] * 7,
            out_specs=pl.BlockSpec(memory_space=pltpu.VMEM),
            scratch_shapes=[
                pltpu.VMEM((local_rows, columns), jnp.int32),
                pltpu.VMEM((local_blocks, BLK), jnp.float32),
                pltpu.VMEM((fields, local_rows), jnp.float32),
                pltpu.VMEM((fields, local_rows), jnp.float32),
                pltpu.VMEM((local_blocks, BLK), jnp.float32),
                pltpu.VMEM((1, block_gene.shape[0]), jnp.int32),
                pltpu.VMEM((1, genes), jnp.int32),
                pltpu.VMEM((fields // 2, 4 * local_rows), jnp.float32),
                pltpu.VMEM((samp_size, fields // 2, 4 * local_rows), jnp.float32),
                pltpu.VMEM((samp_size * local_rows, owned * BLK), jnp.int32),
                pltpu.VMEM((BLK + 16, fields * BLK), jnp.bfloat16),
                pltpu.VMEM((fields, BLK), jnp.float32),
                pltpu.VMEM((fields, BLK), jnp.float32),
                pltpu.VMEM((chunks, fields // 2, BLK), jnp.float32),
                pltpu.VMEM((owned, BLK, BLK), jnp.float32),
                pltpu.VMEM((1, width), jnp.float32),
                pltpu.VMEM((devices, 1, width), jnp.float32),
                pltpu.SemaphoreType.DMA((7,)),
                pltpu.SemaphoreType.DMA((2,)),
                pltpu.SemaphoreType.DMA((samp_size,)),
                pltpu.SemaphoreType.DMA((samp_size,)),
                pltpu.SemaphoreType.DMA,
                pltpu.SemaphoreType.DMA,
                pltpu.SemaphoreType.REGULAR((samp_size,)),
                pltpu.SemaphoreType.REGULAR,
            ],
            compiler_params=pltpu.CompilerParams(collective_id=0, has_side_effects=True),
        )(
            genotypes,
            allele_freq.reshape(local_blocks, BLK),
            sample_weight,
            residual,
            variant_weight.reshape(local_blocks, BLK),
            block_gene.reshape(1, -1),
            gene_variants.reshape(1, -1),
        )
        return both[0], both[1]

    placed = (P("samp", "gene"), P("gene"), P(None, "samp"), P(None, "samp"), P("gene"), P(), P())
    return jax.shard_map(local, mesh=mesh, in_specs=placed, out_specs=(P(), P()), check_vma=False)
```
